32 devices in a mesh: fsdp: 16 (over z, x, core), tp: 2 (over y).
Axes of the slice: x: 2, y: 2, z: 4, core: 2. Of those that a mesh axis runs over, the one named last changes fastest.
Arguments:
- saved_master: float32 [16384, 5120], P(('fsdp', 'tp')), may hold values from -6 to 6
- saved_first: float32 [16384, 5120], P(('fsdp', 'tp')), may hold values from -6 to 6
- saved_second: float32 [16384, 5120], P(('fsdp', 'tp')), may hold values from 0.05 to 20
- grad: bfloat16 [16384, 5120], P('fsdp', 'tp'), may hold values from -10000 to 10000
- row_target: int32 [16384], replicated, may hold values from 0 to 16383, as said below
- step: int32 [1], replicated, may hold values from 1 to 63
Outputs:
- new_master: float32 [16384, 5120], P('fsdp', 'tp')
- new_first: float32 [16384, 5120], P('fsdp', 'tp')
- new_second: float32 [16384, 5120], P('fsdp', 'tp')
- direction: float32 [16384, 5120], P('fsdp', 'tp')
The draws below stay inside these ranges and needn't reach their ends.
Inputs may be any that keep to these rules, and one draw needn't show every extreme that they name: `row_target`: a permutation of 0 to 16383; the saved rows j * 1024 to (j + 1) * 1024 - 1 of every block j send exactly 64 rows into every new block of 1024 rows.
All inputs are finite; a program needn't handle non-finite values.
Results may differ from the reference program's by a relative error of at most 0.0003.
Values sent between devices are 32-bit elements; how exact they have to be, the bound alone decides.
A program may use at most 192 MiB of HBM per device.

```python
import math
import jax
import jax.numpy as jnp

H = 16384
D = 5120
N_FSDP = 16


def draw_row_target(key, part):
    block_rows = H // N_FSDP
    pair_rows = block_rows // N_FSDP
    source_keys = jax.random.split(jax.random.fold_in(key, 11), N_FSDP)
    target_keys = jax.random.split(jax.random.fold_in(key, 12), N_FSDP)
    sigma = jax.vmap(lambda one: jax.random.permutation(one, block_rows))(source_keys).astype(jnp.int32)
    tau_table = jax.vmap(lambda one: jax.random.permutation(one, block_rows))(target_keys).astype(jnp.int32)
    target_block = sigma // pair_rows
    slot_index = sigma % pair_rows
    incoming = jnp.arange(N_FSDP, dtype=jnp.int32)[:, None] * pair_rows + slot_index
    local_row = tau_table.reshape(-1)[target_block * block_rows + incoming]
    return (target_block * block_rows + local_row).reshape(-1).astype(jnp.int32)


def draw_grad(key, part):
    row_key = jax.random.fold_in(key, 21)
    col_key = jax.random.fold_in(key, 22)
    base_key = jax.random.fold_in(key, 23)
    rising = 1.0 + 2.0 * jnp.arange(H, dtype=jnp.float32) / (H - 1)
    row_scale = jnp.exp(jax.random.uniform(row_key, (H, 1)) * math.log(10.0)) * rising[:, None]
    col_scale = jnp.exp(jax.random.uniform(col_key, (1, D)) * math.log(10.0))
    values = jax.random.normal(base_key, (H, D))
    return (values * row_scale * col_scale).astype(jnp.bfloat16)


def level_of(key, extent, cuts, low, largest):
    factor_of, own = 1.0, jax.random.fold_in(key, 6)
    for position, shards_of in cuts:
        heights = jnp.exp(jax.random.uniform(jax.random.fold_in(own, position), (shards_of,), jnp.float32, low / len(cuts), largest / len(cuts)))
        factor_of = factor_of * jnp.repeat(heights, extent[position] // shards_of).reshape([-1 if axis == position else 1 for axis in range(len(extent))])
    return factor_of


def scatter_about(stream_key, dims, deviation, reach, cuts=(), kind=jnp.bfloat16):
    array = jax.random.normal(stream_key, dims, jnp.float32) * deviation
    if len(cuts) > 0:
        array = level_of(stream_key, dims, cuts, -0.22, 0.18) * array
    return jnp.clip(array, min=-reach, max=reach).astype(kind)


def setup_inputs(seed: int = 0) -> dict:
    key_list = jax.random.split(jax.random.key(seed), 7)
    saved_master = scatter_about(key_list[0], (H, D), 1.0, 6.0, ((0, 32),), jnp.float32)
    saved_first = scatter_about(key_list[1], (H, D), 1.0, 6.0, ((0, 32),), jnp.float32)
    saved_second = jnp.clip(jnp.exp(math.log(20.0) - 5.9914645 * jax.random.uniform(key_list[2], (H, D), jnp.float32) ** level_of(key_list[2], (H, D), ((0, 32),), -0.2, 0.2)), 0.05, 20.0)
    grad = draw_grad(jax.random.fold_in(key_list[6], 71), 0)
    row_target = draw_row_target(jax.random.fold_in(key_list[6], 71), 0)
    step = jax.random.randint(key_list[5], (1,), 1, 64).astype(jnp.int32)
    return dict(saved_master=saved_master, saved_first=saved_first, saved_second=saved_second, grad=grad, row_target=row_target, step=step)


beta_one = 0.9
beta_two = 0.95
epsilon = 1e-08
learn_rate = 0.001
weight_decay = 0.1

def adam_update(master, first, second, grad, scale, step):
    clipped = scale * grad.astype(jnp.float32)
    first_new = beta_one * first + (1.0 - beta_one) * clipped
    second_new = beta_two * second + (1.0 - beta_two) * clipped * clipped
    count = step[0].astype(jnp.float32)
    first_hat = first_new / (1.0 - jnp.power(jnp.float32(beta_one), count))
    second_hat = second_new / (1.0 - jnp.power(jnp.float32(beta_two), count))
    direction = first_hat / (jnp.sqrt(second_hat) + epsilon) + weight_decay * master
    return (master - learn_rate * direction, first_new, second_new, direction)

def reference(saved_master, saved_first, saved_second, grad, row_target, step):
    master = jnp.zeros_like(saved_master).at[row_target].set(saved_master)
    first = jnp.zeros_like(saved_first).at[row_target].set(saved_first)
    second = jnp.zeros_like(saved_second).at[row_target].set(saved_second)
    grad_wide = grad.astype(jnp.float32)
    total = jnp.sum(grad_wide * grad_wide)
    scale = jnp.minimum(1.0, math.sqrt(H * D) / jnp.sqrt(total))
    return adam_update(master, first, second, grad, scale, step)
```

```python
import math

import jax
import jax.numpy as jnp
from jax import lax
from jax.experimental import pallas as pl
from jax.experimental.pallas import tpu as pltpu
from jax.sharding import PartitionSpec as P

beta_one = 0.9
beta_two = 0.95
epsilon = 1e-08
learn_rate = 0.001
weight_decay = 0.1

LANES = 128
WEIGHTS = (2, 3, 5, 6, 4)


def adam_kernel(scalars, master_ref, first_ref, second_ref, grad_ref, *refs):
    master_out, first_out, second_out, direction_out = refs[-4:]
    scale, first_fix, second_fix = scalars[0], scalars[1], scalars[2]
    clipped = scale * grad_ref[...].astype(jnp.float32)
    first_new = beta_one * first_ref[...] + (1.0 - beta_one) * clipped
    second_new = beta_two * second_ref[...] + (1.0 - beta_two) * clipped * clipped
    master = master_ref[...]
    first_hat = first_new / first_fix
    second_hat = second_new / second_fix
    direction = first_hat / (jnp.sqrt(second_hat) + epsilon) + weight_decay * master
    master_out[...] = master - learn_rate * direction
    first_out[...] = first_new
    second_out[...] = second_new
    direction_out[...] = direction


def adam_chunk(scalars, placed, grad, outs, begin, end):
    rows, columns = grad.shape
    unit = LANES if columns % LANES == 0 else columns
    count, first_unit = (end - begin) // unit, begin // unit

    def moved(shift):
        return pl.BlockSpec((rows, unit), lambda j: (0, j + shift))

    earlier = () if outs is None else tuple(outs)
    size = rows * (end - begin)
    return pl.pallas_call(
        adam_kernel,
        grid=(count,),
        out_shape=[jax.ShapeDtypeStruct((rows, columns), jnp.float32)] * 4,
        in_specs=[pl.BlockSpec(memory_space=pltpu.SMEM)]
        + [moved(0), moved(count), moved(2 * count), moved(first_unit)]
        + [pl.BlockSpec(memory_space=pl.ANY)] * len(earlier),
        out_specs=[moved(first_unit)] * 4,
        input_output_aliases={5 + i: i for i in range(len(earlier))},
        cost_estimate=pl.CostEstimate(
            flops=16 * size, bytes_accessed=30 * size, transcendentals=2 * size
        ),
        name="adam",
    )(scalars, placed, placed, placed, grad, *earlier)


def column_chunks(columns):
    unit = LANES if columns % LANES == 0 else 1
    units = columns // unit
    total, reached, edges = sum(WEIGHTS), 0, [0]
    for weight in WEIGHTS:
        reached += weight
        edge = units * reached // total
        if edge > edges[-1]:
            edges.append(edge)
    return [(a * unit, b * unit) for a, b in zip(edges[:-1], edges[1:])]


def per_device(all_rows_total, saved_master, saved_first, saved_second, grad, row_target, step):
    tp_count = lax.axis_size("tp")
    tp_index = lax.axis_index("tp")
    block_index = lax.axis_index("fsdp")
    block_rows, columns = grad.shape
    piece_rows = saved_master.shape[0]
    all_rows = row_target.shape[0]
    saved = (saved_master, saved_first, saved_second)

    mine = lax.dynamic_slice_in_dim(row_target, block_index * block_rows, block_rows)
    send_order = jnp.argsort(mine, stable=True)
    owner = send_order // piece_rows
    send_local = jnp.mod(tp_index - owner, tp_count) * piece_rows + send_order % piece_rows

    in_block = row_target // block_rows == block_index
    sort_keys = jnp.where(in_block, row_target, all_rows)
    source_block = jnp.argsort(sort_keys, stable=True)[:block_rows] // block_rows
    local = jnp.arange(block_rows, dtype=jnp.int32)
    before = (source_block[None, :] == source_block[:, None]) & (local[None, :] < local[:, None])
    pair_rows = block_rows // lax.axis_size("fsdp")
    place_order = source_block * pair_rows + jnp.sum(before.astype(jnp.int32), axis=1)

    def part_of(which, begin, end):
        options = [
            jnp.concatenate(
                [x[:, t * columns + begin : t * columns + end] for x in saved], axis=1
            )
            for t in range(tp_count)
        ]
        result = options[0]
        for t in range(1, tp_count):
            result = jnp.where(which == t, options[t], result)
        return result

    chunks = column_chunks(columns)
    middles = []
    for begin, end in chunks:
        pieces = [part_of(tp_index, begin, end)]
        for shift in range(1, tp_count):
            pairs = [(t, (t + shift) % tp_count) for t in range(tp_count)]
            outgoing = part_of(jnp.mod(tp_index + shift, tp_count), begin, end)
            pieces.append(lax.ppermute(outgoing, "tp", pairs))
        middles.append(pieces)

    grad_wide = grad.astype(jnp.float32)
    squares = lax.all_gather(jnp.sum(grad_wide * grad_wide), ("fsdp", "tp"))
    total = jnp.sum(squares)
    scale = jnp.minimum(1.0, math.sqrt(all_rows_total) / jnp.sqrt(total))

    count = step[0].astype(jnp.float32)
    scalars = jnp.stack(
        [
            scale,
            1.0 - jnp.power(jnp.float32(beta_one), count),
            1.0 - jnp.power(jnp.float32(beta_two), count),
        ]
    )
    arrived, updated = [], []
    for index, pieces in enumerate(middles):
        gathered = jnp.concatenate(pieces, axis=0)[send_local]
        if index >= 2:
            placed = arrived[index - 2][place_order]
            earlier = updated[-1] if updated else None
            updated.append(adam_chunk(scalars, placed, grad, earlier, *chunks[index - 2]))
            gathered, arrived[-1], updated[-1] = lax.optimization_barrier(
                (gathered, arrived[-1], updated[-1])
            )
        elif index == 1:
            gathered, arrived[0] = lax.optimization_barrier((gathered, arrived[0]))
        arrived.append(
            lax.all_to_all(gathered, "fsdp", split_axis=0, concat_axis=0, tiled=True)
        )
    for index in range(len(updated), len(chunks)):
        placed = arrived[index][place_order]
        earlier = updated[-1] if updated else None
        updated.append(adam_chunk(scalars, placed, grad, earlier, *chunks[index]))
    return tuple(updated[-1])


def solution(mesh):
    in_specs = (
        P(("fsdp", "tp"), None),
        P(("fsdp", "tp"), None),
        P(("fsdp", "tp"), None),
        P("fsdp", "tp"),
        P(),
        P(),
    )
    out_specs = (P("fsdp", "tp"), P("fsdp", "tp"), P("fsdp", "tp"), P("fsdp", "tp"))

    def whole(saved_master, saved_first, saved_second, grad, row_target, step):
        def body(*args):
            return per_device(grad.shape[0] * grad.shape[1], *args)

        return jax.shard_map(
            body, mesh=mesh, in_specs=in_specs, out_specs=out_specs, check_vma=False
        )(saved_master, saved_first, saved_second, grad, row_target, step)

    return whole
```

```python
import math

import jax
import jax.numpy as jnp
from jax import lax
from jax.experimental import pallas as pl
from jax.experimental.pallas import tpu as pltpu
from jax.sharding import PartitionSpec as P

beta_one = 0.9
beta_two = 0.95
epsilon = 1e-08
learn_rate = 0.001
weight_decay = 0.1

LANES = 128
WEIGHTS = (2, 3, 4, 5, 4, 2)


def adam_kernel(scalars, master_ref, first_ref, second_ref, grad_ref, *refs):
    master_out, first_out, second_out, direction_out = refs[-4:]
    scale, first_fix, second_fix = scalars[0], scalars[1], scalars[2]
    clipped = scale * grad_ref[...].astype(jnp.float32)
    first_new = beta_one * first_ref[...] + (1.0 - beta_one) * clipped
    second_new = beta_two * second_ref[...] + (1.0 - beta_two) * clipped * clipped
    master = master_ref[...]
    first_hat = first_new / first_fix
    second_hat = second_new / second_fix
    direction = first_hat / (jnp.sqrt(second_hat) + epsilon) + weight_decay * master
    master_out[...] = master - learn_rate * direction
    first_out[...] = first_new
    second_out[...] = second_new
    direction_out[...] = direction


def adam_chunk(scalars, placed, grad, outs, begin, end):
    rows, columns = grad.shape
    unit = LANES if columns % LANES == 0 else columns
    count, first_unit = (end - begin) // unit, begin // unit

    def moved(shift):
        return pl.BlockSpec((rows, unit), lambda j: (0, j + shift))

    earlier = () if outs is None else tuple(outs)
    size = rows * (end - begin)
    return pl.pallas_call(
        adam_kernel,
        grid=(count,),
        out_shape=[jax.ShapeDtypeStruct((rows, columns), jnp.float32)] * 4,
        in_specs=[pl.BlockSpec(memory_space=pltpu.SMEM)]
        + [moved(0), moved(count), moved(2 * count), moved(first_unit)]
        + [pl.BlockSpec(memory_space=pl.ANY)] * len(earlier),
        out_specs=[moved(first_unit)] * 4,
        input_output_aliases={5 + i: i for i in range(len(earlier))},
        cost_estimate=pl.CostEstimate(
            flops=16 * size, bytes_accessed=30 * size, transcendentals=2 * size
        ),
        name="adam",
    )(scalars, placed, placed, placed, grad, *earlier)


def column_chunks(columns):
    unit = LANES if columns % LANES == 0 else 1
    units = columns // unit
    total, reached, edges = sum(WEIGHTS), 0, [0]
    for weight in WEIGHTS:
        reached += weight
        edge = units * reached // total
        if edge > edges[-1]:
            edges.append(edge)
    return [(a * unit, b * unit) for a, b in zip(edges[:-1], edges[1:])]


def per_device(all_rows_total, saved_master, saved_first, saved_second, grad, row_target, step):
    tp_count = lax.axis_size("tp")
    tp_index = lax.axis_index("tp")
    block_index = lax.axis_index("fsdp")
    block_rows, columns = grad.shape
    piece_rows = saved_master.shape[0]
    all_rows = row_target.shape[0]
    saved = (saved_master, saved_first, saved_second)

    mine = lax.dynamic_slice_in_dim(row_target, block_index * block_rows, block_rows)
    send_order = jnp.argsort(mine, stable=True)
    owner = send_order // piece_rows
    send_local = jnp.mod(tp_index - owner, tp_count) * piece_rows + send_order % piece_rows

    in_block = row_target // block_rows == block_index
    sort_keys = jnp.where(in_block, row_target, all_rows)
    source_block = jnp.argsort(sort_keys, stable=True)[:block_rows] // block_rows
    local = jnp.arange(block_rows, dtype=jnp.int32)
    before = (source_block[None, :] == source_block[:, None]) & (local[None, :] < local[:, None])
    pair_rows = block_rows // lax.axis_size("fsdp")
    place_order = source_block * pair_rows + jnp.sum(before.astype(jnp.int32), axis=1)

    def part_of(which, begin, end):
        options = [
            jnp.concatenate(
                [x[:, t * columns + begin : t * columns + end] for x in saved], axis=1
            )
            for t in range(tp_count)
        ]
        result = options[0]
        for t in range(1, tp_count):
            result = jnp.where(which == t, options[t], result)
        return result

    chunks = column_chunks(columns)
    shifts = range(1, tp_count)
    leaving = [
        [part_of(jnp.mod(tp_index + shift, tp_count), begin, end) for shift in shifts]
        for begin, end in chunks
    ]
    middles = []
    for index, (begin, end) in enumerate(chunks):
        pieces = [part_of(tp_index, begin, end)]
        for shift, outgoing in zip(shifts, leaving[index]):
            pairs = [(t, (t + shift) % tp_count) for t in range(tp_count)]
            pieces.append(lax.ppermute(outgoing, "tp", pairs))
        if index + 1 < len(chunks):
            pieces, leaving[index + 1] = lax.optimization_barrier((pieces, leaving[index + 1]))
        middles.append(pieces)

    grad_wide = grad.astype(jnp.float32)
    squares = lax.all_gather(jnp.sum(grad_wide * grad_wide), ("fsdp", "tp"))
    total = jnp.sum(squares)
    scale = jnp.minimum(1.0, math.sqrt(all_rows_total) / jnp.sqrt(total))

    count = step[0].astype(jnp.float32)
    scalars = jnp.stack(
        [
            scale,
            1.0 - jnp.power(jnp.float32(beta_one), count),
            1.0 - jnp.power(jnp.float32(beta_two), count),
        ]
    )
    arrived, updated = [], []
    for index, pieces in enumerate(middles):
        gathered = jnp.concatenate(pieces, axis=0)[send_local]
        if index == 0:
            gathered, scalars = lax.optimization_barrier((gathered, scalars))
        if index >= 2:
            placed = arrived[index - 2][place_order]
            earlier = updated[-1] if updated else None
            updated.append(adam_chunk(scalars, placed, grad, earlier, *chunks[index - 2]))
            gathered, arrived[-1], updated[-1] = lax.optimization_barrier(
                (gathered, arrived[-1], updated[-1])
            )
        elif index == 1:
            gathered, arrived[0] = lax.optimization_barrier((gathered, arrived[0]))
        arrived.append(
            lax.all_to_all(gathered, "fsdp", split_axis=0, concat_axis=0, tiled=True)
        )
    for index in range(len(updated), len(chunks)):
        placed = arrived[index][place_order]
        earlier = updated[-1] if updated else None
        updated.append(adam_chunk(scalars, placed, grad, earlier, *chunks[index]))
    return tuple(updated[-1])


def solution(mesh):
    in_specs = (
        P(("fsdp", "tp"), None),
        P(("fsdp", "tp"), None),
        P(("fsdp", "tp"), None),
        P("fsdp", "tp"),
        P(),
        P(),
    )
    out_specs = (P("fsdp", "tp"), P("fsdp", "tp"), P("fsdp", "tp"), P("fsdp", "tp"))

    def whole(saved_master, saved_first, saved_second, grad, row_target, step):
        def body(*args):
            return per_device(grad.shape[0] * grad.shape[1], *args)

        return jax.shard_map(
            body, mesh=mesh, in_specs=in_specs, out_specs=out_specs, check_vma=False
        )(saved_master, saved_first, saved_second, grad, row_target, step)

    return whole
```
